32 devices in a mesh: row: 8 (over y, x, core), col: 4 (over z).
Axes of the slice: x: 2, y: 2, z: 4, core: 2. Of those that a mesh axis runs over, the one named last changes fastest.
Arguments:
- factor_a: bfloat16 [128, 32768], P('row', 'col'), may hold values from -12 to 12
- factor_b: bfloat16 [128, 32768], P('row', 'col'), may hold values from -12 to 12
- pair: bfloat16 [1024, 1024, 128], P('row', 'col'), may hold values from -6 to 6
- proj_weight: bfloat16 [1024, 128], replicated, may hold values from -0.1875 to 0.1875
- proj_bias: float32 [128], replicated, may hold values from -3 to 3
- norm_gain: float32 [128], replicated, may hold values from 0.25 to 1.75
- norm_bias: float32 [128], replicated, may hold values from -3 to 3
- trans_in: bfloat16 [128, 1024], replicated, may hold values from -0.5 to 0.5
- trans_out: bfloat16 [512, 128], replicated, may hold values from -0.25 to 0.25
- cotangent: bfloat16 [1024, 1024, 128], P('row', 'col'), may hold values from -6 to 6
Outputs:
- new_pair: bfloat16 [1024, 1024, 128], P('row', 'col')
- pair_grad: bfloat16 [1024, 1024, 128], P('row', 'col')
- grad_a: float32 [128, 32768], P('row', 'col')
- grad_b: float32 [128, 32768], P('row', 'col')
The draws below stay inside these ranges and needn't reach their ends.
All inputs are finite; a program needn't handle non-finite values.
Results may differ from the reference program's by a relative error of at most 0.006.
Values may be sent and summed in bfloat16 or wider, within the bound.
No kernel may reach another device: no remote copies, remote signals or barrier semaphores. Data moves between devices by JAX's collectives and lax.ppermute only.
A program may use at most 128 MiB of HBM per device.

```python
import jax
import jax.numpy as jnp
from jax import lax

H = 32
C = 128
F = 512
S = 128
R = 1024


def block_scale(own_key, dims, cuts, smallest, high):
    def one(position, shards_of):
        heights = jax.random.uniform(jax.random.fold_in(jax.random.fold_in(own_key, 6), position), (shards_of,), jnp.float32, smallest / len(cuts), high / len(cuts))
        return jnp.repeat(jnp.exp(heights), dims[position] // shards_of).reshape((-1,) + (1,) * (len(dims) - position - 1))

    level = one(*cuts[0])
    for cut in cuts[1:]:
        level = level * one(*cut)
    return level


def bell_draw(rng, dims, scale, bound, pieces=(), held_as=jnp.bfloat16):
    factor_of = block_scale(rng, dims, pieces, -0.22, 0.18) if pieces else 1.0
    drawn = jax.random.normal(rng, dims, jnp.float32) * scale * factor_of
    return jnp.minimum(jnp.maximum(drawn, -bound), bound).astype(held_as)


def setup_inputs(seed: int = 0) -> dict:
    streams_of = jax.random.split(jax.random.key(seed), 11)
    factor_a = bell_draw(streams_of[0], (S, R * H), 2.0, 12.0, ((0, 8), (1, 4)))
    factor_b = bell_draw(streams_of[1], (S, R * H), 2.0, 12.0, ((0, 8), (1, 4)))
    pair = bell_draw(streams_of[2], (R, R, C), 1.0, 6.0, ((0, 8), (1, 4)))
    proj_weight = bell_draw(streams_of[3], (H * H, C), (H * H) ** -0.5, 0.1875)
    proj_bias = bell_draw(streams_of[4], (C,), 0.5, 3.0, (), jnp.float32)
    norm_gain = jnp.clip(1.0 + 0.15 * jax.random.normal(streams_of[5], (C,), jnp.float32), 0.25, 1.75)
    norm_bias = bell_draw(streams_of[6], (C,), 0.5, 3.0, (), jnp.float32)
    trans_in = bell_draw(streams_of[7], (C, 2 * F), C ** -0.5, 0.5)
    trans_out = bell_draw(streams_of[8], (F, C), F ** -0.5, 0.25)
    cotangent = bell_draw(streams_of[9], (R, R, C), 1.0, 6.0, ((0, 8), (1, 4)))
    return dict(factor_a=factor_a, factor_b=factor_b, pair=pair, proj_weight=proj_weight, proj_bias=proj_bias, norm_gain=norm_gain, norm_bias=norm_bias, trans_in=trans_in, trans_out=trans_out, cotangent=cotangent)


def dot_last(left, right):
    return lax.dot_general(left, right, (((1,), (1,)), ((), ())), preferred_element_type=jnp.float32)

def dot_first(left, right):
    return lax.dot_general(left, right, (((0,), (0,)), ((), ())), preferred_element_type=jnp.float32)

def factor_pull(grad_rows, proj_weight, seq_count, hidden_dim):
    rows_i, cols_j, width = grad_rows.shape
    weight_cube = proj_weight.reshape(hidden_dim, hidden_dim, width).astype(jnp.float32)
    pulled = jnp.einsum('abc,hkc->ahbk', grad_rows.astype(jnp.float32), weight_cube) / seq_count
    pulled = pulled.astype(jnp.bfloat16)
    return pulled.reshape(rows_i * hidden_dim, cols_j * hidden_dim)

def pair_update(a_block, b_cols, pair_rows, cot_rows, proj_weight, proj_bias, norm_gain, norm_bias, trans_in, trans_out, seq_count, hidden_dim):
    rows_i, cols_j, width = pair_rows.shape
    units = trans_out.shape[0]
    outer = (dot_first(a_block, b_cols) / seq_count).astype(jnp.bfloat16)
    outer = outer.reshape(rows_i, hidden_dim, cols_j, hidden_dim).astype(jnp.float32)
    weight_cube = proj_weight.reshape(hidden_dim, hidden_dim, width).astype(jnp.float32)
    projected = jnp.einsum('ahbk,hkc->abc', outer, weight_cube).reshape(rows_i * cols_j, width)
    updated = pair_rows.reshape(rows_i * cols_j, width).astype(jnp.float32)
    updated = updated + projected + proj_bias
    row_mean = lax.optimization_barrier(jnp.mean(updated, axis=-1, keepdims=True))
    centered = updated - row_mean
    row_var = lax.optimization_barrier(jnp.mean(centered * centered, axis=-1, keepdims=True))
    inv_std = lax.rsqrt(row_var + 1e-05)
    normed = centered * inv_std
    lnorm = (normed * norm_gain + norm_bias).astype(jnp.bfloat16)
    both_pre = jnp.dot(lnorm, trans_in, preferred_element_type=jnp.float32)
    gate_pre = both_pre[:, :units]
    up_pre = both_pre[:, units:]
    sig_gate = jax.nn.sigmoid(gate_pre)
    activated = gate_pre * sig_gate
    hidden = (activated * up_pre).astype(jnp.bfloat16)
    new_rows = (updated + jnp.dot(hidden, trans_out, preferred_element_type=jnp.float32)).astype(jnp.bfloat16)
    cot_flat = cot_rows.reshape(rows_i * cols_j, width)
    d_hidden = dot_last(cot_flat, trans_out)
    d_gate = d_hidden * up_pre * sig_gate * (1.0 + gate_pre * (1.0 - sig_gate))
    d_up = d_hidden * activated
    d_both = jnp.concatenate([d_gate, d_up], axis=-1).astype(jnp.bfloat16)
    d_norm = dot_last(d_both, trans_in) * norm_gain
    d_mean = lax.optimization_barrier(jnp.mean(d_norm, axis=-1, keepdims=True))
    d_proj = lax.optimization_barrier(jnp.mean(d_norm * normed, axis=-1, keepdims=True))
    grad_flat = cot_flat.astype(jnp.float32) + inv_std * (d_norm - d_mean - normed * d_proj)
    grad_rows = grad_flat.astype(jnp.bfloat16).reshape(rows_i, cols_j, width)
    pulled = factor_pull(grad_rows, proj_weight, seq_count, hidden_dim)
    return (new_rows.reshape(rows_i, cols_j, width), grad_rows, pulled)

def reference(factor_a, factor_b, pair, proj_weight, proj_bias, norm_gain, norm_bias, trans_in, trans_out, cotangent):
    blocks = 32
    rows_block = R // blocks
    a_blocks = factor_a.reshape(S, blocks, rows_block * H).transpose(1, 0, 2)
    pair_blocks = pair.reshape(blocks, rows_block, R, C)
    cot_blocks = cotangent.reshape(blocks, rows_block, R, C)

    def advance(running, inputs_now):
        a_block, pair_rows, cot_rows = inputs_now
        new_rows, grad_rows, pulled = pair_update(a_block, factor_b, pair_rows, cot_rows, proj_weight, proj_bias, norm_gain, norm_bias, trans_in, trans_out, S, H)
        grad_a_block = dot_last(factor_b, pulled)
        running = running + jnp.dot(a_block, pulled, preferred_element_type=jnp.float32)
        return (running, (new_rows, grad_rows, grad_a_block))
    start_sum = jnp.zeros((S, R * H), jnp.float32)
    grad_b, outputs = lax.scan(advance, start_sum, (a_blocks, pair_blocks, cot_blocks))
    new_stack, grad_stack, part_stack = outputs
    new_pair = new_stack.reshape(R, R, C)
    pair_grad = grad_stack.reshape(R, R, C)
    grad_a = part_stack.transpose(1, 0, 2).reshape(S, R * H)
    return (new_pair, pair_grad, grad_a, grad_b)
```

```python
import functools

import jax
import jax.numpy as jnp
from jax import lax
from jax.experimental import pallas as pl
from jax.experimental.pallas import tpu as pltpu
from jax.sharding import PartitionSpec as P

H = 32
F32 = jnp.float32
BF16 = jnp.bfloat16


def mm(left, right):
    return lax.dot_general(
        left, right, (((1,), (0,)), ((), ())), preferred_element_type=F32
    )


def mm_nt(left, right):
    return lax.dot_general(
        left, right, (((1,), (1,)), ((), ())), preferred_element_type=F32
    )


def pair_kernel(
    a_ref,
    b_ref,
    pair_ref,
    cot_ref,
    proj_t_ref,
    proj_ref,
    wide_ref,
    out_t_ref,
    in_ref,
    vec_ref,
    new_ref,
    grad_ref,
    ga_ref,
    gb_ref,
    outer_s,
    pulled_s,
    hidden_s,
    both_s,
    rhs_s,
    *,
    unit_chunk,
):
    seqs = a_ref.shape[0]
    rows, cols, width = pair_ref.shape
    units = out_t_ref.shape[1]
    inv_seqs = 1.0 / seqs

    @pl.when(pl.program_id(0) == 0)
    def _():
        gb_ref[...] = jnp.zeros_like(gb_ref)

    a_t = a_ref[...].T
    for h in range(H):
        outer = mm(a_t, b_ref[:, h * cols : (h + 1) * cols])
        outer_s[:, h * H : (h + 1) * H, :] = outer.astype(BF16).reshape(rows, H, cols)
    for i in range(rows):
        projected = mm(proj_t_ref[...], outer_s[i])
        updated = pair_ref[i].T.astype(F32) + (projected * inv_seqs + vec_ref[0])
        mean = jnp.mean(updated, axis=0, keepdims=True)
        centered = updated - mean
        var = jnp.mean(centered * centered, axis=0, keepdims=True)
        inv_std = lax.rsqrt(var + 1e-05)
        normed = centered * inv_std
        rhs_s[:width, :] = (normed * vec_ref[1] + vec_ref[2]).astype(BF16)
        rhs_s[width:, :] = cot_ref[i].T
        rhs = rhs_s[...]
        for u in range(0, units, unit_chunk):
            gate = mm(wide_ref[u : u + unit_chunk, :], rhs)
            up = mm(wide_ref[units + u : units + u + unit_chunk, :], rhs)
            d_hid = mm(wide_ref[2 * units + u : 2 * units + u + unit_chunk, :], rhs)
            sig = 0.5 * jnp.tanh(0.5 * gate) + 0.5
            act = gate * sig
            hidden_s[u : u + unit_chunk, :] = (act * up).astype(BF16)
            both_s[units + u : units + u + unit_chunk, :] = (d_hid * act).astype(BF16)
            both_s[u : u + unit_chunk, :] = (d_hid * up * (sig + act * (1.0 - sig))).astype(BF16)
        new_t = updated + mm(out_t_ref[...], hidden_s[...])
        new_ref[i] = new_t.astype(BF16).T
        d_norm = mm(in_ref[...], both_s[...]) * vec_ref[1]
        d_mean = jnp.mean(d_norm, axis=0, keepdims=True)
        d_proj = jnp.mean(d_norm * normed, axis=0, keepdims=True)
        grad_t = rhs_s[width:, :].astype(F32) + inv_std * (d_norm - d_mean - normed * d_proj)
        grad_t = grad_t.astype(BF16)
        grad_ref[i] = grad_t.T
        pulled_s[i] = mm(proj_ref[...], grad_t).astype(BF16)
    ga = jnp.zeros((rows * H, seqs), F32)
    for h in range(H):
        tile = pulled_s[:, h * H : (h + 1) * H, :].reshape(rows * H, cols)
        ga = ga + mm_nt(tile, b_ref[:, h * cols : (h + 1) * cols])
        gb_ref[:, h * cols : (h + 1) * cols] += mm(a_ref[...], tile)
    ga_ref[...] = ga.T


def pair_tile(a_own, b_cols, pair, cot, weights, block_rows, unit_chunk):
    seqs = a_own.shape[0]
    rows, cols, width = pair.shape
    units = weights[3].shape[1]

    def whole(array):
        return pl.BlockSpec(array.shape, lambda b: (0,) * array.ndim)

    pair_spec = pl.BlockSpec((block_rows, cols, width), lambda b: (b, 0, 0))
    a_spec = pl.BlockSpec((seqs, block_rows * H), lambda b: (0, b))
    return pl.pallas_call(
        functools.partial(pair_kernel, unit_chunk=unit_chunk),
        grid=(rows // block_rows,),
        in_specs=[a_spec, whole(b_cols), pair_spec, pair_spec] + [whole(w) for w in weights],
        out_specs=[pair_spec, pair_spec, a_spec, pl.BlockSpec((seqs, H * cols), lambda b: (0, 0))],
        out_shape=[
            jax.ShapeDtypeStruct((rows, cols, width), BF16),
            jax.ShapeDtypeStruct((rows, cols, width), BF16),
            jax.ShapeDtypeStruct((seqs, rows * H), F32),
            jax.ShapeDtypeStruct((seqs, H * cols), F32),
        ],
        scratch_shapes=[
            pltpu.VMEM((block_rows, H * H, cols), BF16),
            pltpu.VMEM((block_rows, H * H, cols), BF16),
            pltpu.VMEM((units, cols), BF16),
            pltpu.VMEM((2 * units, cols), BF16),
            pltpu.VMEM((2 * width, cols), BF16),
        ],
        compiler_params=pltpu.CompilerParams(
            dimension_semantics=("arbitrary",), vmem_limit_bytes=60 * 2**20
        ),
    )(a_own, b_cols, pair, cot, *weights)


def kernel_weights(proj_weight, proj_bias, norm_gain, norm_bias, trans_in, trans_out, cols):
    width = proj_weight.shape[1]
    units = trans_out.shape[0]
    proj = proj_weight.reshape(H, H, width).transpose(1, 0, 2).reshape(H * H, width)
    wide = jnp.concatenate(
        [
            jnp.concatenate([trans_in.T, jnp.zeros((2 * units, width), BF16)], axis=1),
            jnp.concatenate([jnp.zeros((units, width), BF16), trans_out], axis=1),
        ],
        axis=0,
    )
    vec = jnp.stack([proj_bias, norm_gain, norm_bias])[:, :, None]
    vec = jnp.broadcast_to(vec, (3, width, cols))
    return proj.T, proj, wide, trans_out.T, trans_in, vec


def body(
    factor_a,
    factor_b,
    pair,
    proj_weight,
    proj_bias,
    norm_gain,
    norm_bias,
    trans_in,
    trans_out,
    cotangent,
):
    rows_here, cols_here, width = pair.shape
    seqs_here = factor_a.shape[0]
    seq_count = seqs_here * lax.axis_size("row")
    cols = -(-cols_here // 128) * 128
    spare = cols - cols_here

    gathered = lax.all_gather(factor_a, "col", axis=1, tiled=True)
    a_own = lax.all_to_all(gathered, "row", split_axis=1, concat_axis=0, tiled=True)
    b_local = factor_b.reshape(seqs_here, cols_here, H).transpose(0, 2, 1)
    b_local = jnp.pad(b_local, ((0, 0), (0, 0), (0, spare))).reshape(seqs_here, H * cols)
    b_cols = lax.all_gather(b_local, "row", axis=0, tiled=True)
    if spare:
        pair = jnp.pad(pair, ((0, 0), (0, spare), (0, 0)))
        cotangent = jnp.pad(cotangent, ((0, 0), (0, spare), (0, 0)))
    weights = kernel_weights(
        proj_weight, proj_bias, norm_gain, norm_bias, trans_in, trans_out, cols
    )
    new_pair, pair_grad, ga_part, gb_part = pair_tile(
        a_own, b_cols, pair, cotangent, weights, 8, 128
    )
    new_pair = new_pair[:, :cols_here]
    pair_grad = pair_grad[:, :cols_here]
    gb_own = lax.psum_scatter(gb_part, "row", scatter_dimension=0, tiled=True)
    gb_own = gb_own.reshape(seqs_here, H, cols)[:, :, :cols_here].transpose(0, 2, 1)
    grad_b = gb_own.reshape(seqs_here, cols_here * H) / seq_count
    returned = lax.all_to_all(ga_part, "row", split_axis=0, concat_axis=1, tiled=True)
    grad_a = lax.psum_scatter(returned, "col", scatter_dimension=1, tiled=True) / seq_count
    return (new_pair, pair_grad, grad_a, grad_b)


def solution(mesh):
    placed = (
        P("row", "col"),
        P("row", "col"),
        P("row", "col", None),
        P(),
        P(),
        P(),
        P(),
        P(),
        P(),
        P("row", "col", None),
    )
    return jax.shard_map(
        body,
        mesh=mesh,
        in_specs=placed,
        out_specs=(P("row", "col", None), P("row", "col", None), P("row", "col"), P("row", "col")),
        check_vma=False,
    )
```

```python
import functools

import jax
import jax.numpy as jnp
from jax import lax
from jax.experimental import pallas as pl
from jax.experimental.pallas import tpu as pltpu
from jax.sharding import PartitionSpec as P

H = 32
F32 = jnp.float32
BF16 = jnp.bfloat16


def mm(left, right):
    return lax.dot_general(
        left, right, (((1,), (0,)), ((), ())), preferred_element_type=F32
    )


def mm_nt(left, right):
    return lax.dot_general(
        left, right, (((1,), (1,)), ((), ())), preferred_element_type=F32
    )


def pair_kernel(place_ref, *refs, ranks, unit_chunk):
    a_pieces, refs = refs[:ranks], refs[ranks:]
    b_pieces, refs = refs[:ranks], refs[ranks:]
    (
        pair_ref,
        cot_ref,
        proj_t_ref,
        proj_ref,
        wide_ref,
        out_t_ref,
        in_ref,
        vec_ref,
        new_ref,
        grad_ref,
        gb_near_ref,
        gb_far_ref,
    ), refs = refs[:12], refs[12:]
    ga_pieces, refs = refs[:ranks], refs[ranks:]
    a_s, b_ref, ga_s, gb_ref, outer_s, pulled_s, hidden_s, both_s, rhs_s = refs
    step = pl.program_id(0)
    seqs = b_ref.shape[0]
    share = seqs // ranks
    rows, cols, width = pair_ref.shape
    units = out_t_ref.shape[1]
    inv_seqs = 1.0 / seqs

    @pl.when(step == 0)
    def _():
        gb_ref[...] = jnp.zeros_like(gb_ref)
        for k in range(ranks):
            b_ref[k * share : (k + 1) * share, :] = b_pieces[k][...]

    for k in range(ranks):
        a_s[pl.ds(pl.multiple_of(place_ref[k] * share, share), share), :] = a_pieces[k][...]
    a_t = a_s[...].T
    for h in range(H):
        outer = mm(a_t, b_ref[:, h * cols : (h + 1) * cols])
        outer_s[:, h * H : (h + 1) * H, :] = outer.astype(BF16).reshape(rows, H, cols)
    for i in range(rows):
        projected = mm(proj_t_ref[...], outer_s[i])
        updated = pair_ref[i].T.astype(F32) + (projected * inv_seqs + vec_ref[0])
        mean = jnp.mean(updated, axis=0, keepdims=True)
        centered = updated - mean
        var = jnp.mean(centered * centered, axis=0, keepdims=True)
        inv_std = lax.rsqrt(var + 1e-05)
        normed = centered * inv_std
        rhs_s[:width, :] = (normed * vec_ref[1] + vec_ref[2]).astype(BF16)
        rhs_s[width:, :] = cot_ref[i].T
        rhs = rhs_s[...]
        for u in range(0, units, unit_chunk):
            gate = mm(wide_ref[u : u + unit_chunk, :], rhs)
            up = mm(wide_ref[units + u : units + u + unit_chunk, :], rhs)
            d_hid = mm(wide_ref[2 * units + u : 2 * units + u + unit_chunk, :], rhs)
            sig = 0.5 * jnp.tanh(0.5 * gate) + 0.5
            act = gate * sig
            hidden_s[u : u + unit_chunk, :] = (act * up).astype(BF16)
            both_s[units + u : units + u + unit_chunk, :] = (d_hid * act).astype(BF16)
            both_s[u : u + unit_chunk, :] = (d_hid * up * (sig + act * (1.0 - sig))).astype(BF16)
        new_t = updated + mm(out_t_ref[...], hidden_s[...])
        new_ref[i] = new_t.astype(BF16).T
        d_norm = mm(in_ref[...], both_s[...]) * vec_ref[1]
        d_mean = jnp.mean(d_norm, axis=0, keepdims=True)
        d_proj = jnp.mean(d_norm * normed, axis=0, keepdims=True)
        grad_t = rhs_s[width:, :].astype(F32) + inv_std * (d_norm - d_mean - normed * d_proj)
        grad_t = grad_t.astype(BF16)
        grad_ref[i] = grad_t.T
        pulled_s[i] = mm(proj_ref[...], grad_t).astype(BF16)
    ga = jnp.zeros((rows * H, seqs), F32)
    for h in range(H):
        tile = pulled_s[:, h * H : (h + 1) * H, :].reshape(rows * H, cols)
        ga = ga + mm_nt(tile, b_ref[:, h * cols : (h + 1) * cols])
        gb_ref[:, h * cols : (h + 1) * cols] += mm(a_s[...], tile)
    ga_s[...] = ga.T.astype(BF16)
    for k in range(ranks):
        ga_pieces[k][...] = ga_s[pl.ds(pl.multiple_of(place_ref[k] * share, share), share), :]

    @pl.when(step == pl.num_programs(0) - 1)
    def _():
        gb_near_ref[...] = gb_ref[: seqs // 2, :]
        gb_far_ref[...] = gb_ref[seqs // 2 :, :].astype(BF16)


def pair_tile(place, a_pieces, b_pieces, pair, cot, weights, block_rows, unit_chunk):
    ranks = len(a_pieces)
    share = a_pieces[0].shape[0]
    seqs = ranks * share
    rows, cols, width = pair.shape
    units = weights[3].shape[1]

    def whole(shape):
        return pl.BlockSpec(shape, lambda b, place: (0,) * len(shape))

    pair_spec = pl.BlockSpec((block_rows, cols, width), lambda b, place: (b, 0, 0))
    a_spec = pl.BlockSpec((share, block_rows * H), lambda b, place: (0, b))
    half = (seqs // 2, H * cols)
    outs = pl.pallas_call(
        functools.partial(pair_kernel, ranks=ranks, unit_chunk=unit_chunk),
        grid_spec=pltpu.PrefetchScalarGridSpec(
            num_scalar_prefetch=1,
            grid=(rows // block_rows,),
            in_specs=[a_spec] * ranks
            + [whole(p.shape) for p in b_pieces]
            + [pair_spec, pair_spec]
            + [whole(w.shape) for w in weights],
            out_specs=[pair_spec, pair_spec, whole(half), whole(half)] + [a_spec] * ranks,
            scratch_shapes=[
                pltpu.VMEM((seqs, block_rows * H), BF16),
                pltpu.VMEM((seqs, H * cols), BF16),
                pltpu.VMEM((seqs, block_rows * H), BF16),
                pltpu.VMEM((seqs, H * cols), F32),
                pltpu.VMEM((block_rows, H * H, cols), BF16),
                pltpu.VMEM((block_rows, H * H, cols), BF16),
                pltpu.VMEM((units, cols), BF16),
                pltpu.VMEM((2 * units, cols), BF16),
                pltpu.VMEM((2 * width, cols), BF16),
            ],
        ),
        out_shape=[
            jax.ShapeDtypeStruct((rows, cols, width), BF16),
            jax.ShapeDtypeStruct((rows, cols, width), BF16),
            jax.ShapeDtypeStruct(half, F32),
            jax.ShapeDtypeStruct(half, BF16),
        ]
        + [jax.ShapeDtypeStruct((share, rows * H), BF16)] * ranks,
        compiler_params=pltpu.CompilerParams(
            dimension_semantics=("arbitrary",), vmem_limit_bytes=60 * 2**20
        ),
    )(place, *a_pieces, *b_pieces, pair, cot, *weights)
    return outs[:4], outs[4:]


def kernel_weights(proj_weight, proj_bias, norm_gain, norm_bias, trans_in, trans_out, cols):
    width = proj_weight.shape[1]
    units = trans_out.shape[0]
    proj = proj_weight.reshape(H, H, width).transpose(1, 0, 2).reshape(H * H, width)
    wide = jnp.concatenate(
        [
            jnp.concatenate([trans_in.T, jnp.zeros((2 * units, width), BF16)], axis=1),
            jnp.concatenate([jnp.zeros((units, width), BF16), trans_out], axis=1),
        ],
        axis=0,
    )
    vec = jnp.stack([proj_bias, norm_gain, norm_bias])[:, :, None]
    vec = jnp.broadcast_to(vec, (3, width, cols))
    return proj.T, proj, wide, trans_out.T, trans_in, vec


def body(
    factor_a,
    factor_b,
    pair,
    proj_weight,
    proj_bias,
    norm_gain,
    norm_bias,
    trans_in,
    trans_out,
    cotangent,
):
    ranks = lax.axis_size("row")
    lines = lax.axis_size("col")
    split = ranks // lines
    row = lax.axis_index("row")
    col = lax.axis_index("col")
    partner = row ^ 1
    rows_here, cols_here, width = pair.shape
    seqs_here = factor_a.shape[0]
    seq_count = seqs_here * ranks
    cols = -(-cols_here // 128) * 128
    spare = cols - cols_here
    near = ranks // 2

    def to_partner(array):
        return lax.ppermute(array, "row", [(r, r ^ 1) for r in range(ranks)])

    def from_ahead(array, k):
        return lax.ppermute(array, "row", [((r + 2 * k) % ranks, r) for r in range(ranks)])

    def block_pairs(k):
        return [
            ((((r % split) * lines + c) ^ k) * lines + r // split, r * lines + c)
            for r in range(ranks)
            for c in range(lines)
        ]

    def flipped(pairs):
        return [(there, here) for here, there in pairs]

    width_a = rows_here * H
    a_pieces = []
    for k in range(ranks):
        which = (row ^ k) // lines
        piece = lax.dynamic_slice_in_dim(factor_a, which * width_a, width_a, 1)
        a_pieces.append(lax.ppermute(piece, ("row", "col"), block_pairs(k)))
    source = ((row % split) * lines + col) ^ jnp.arange(ranks, dtype=jnp.int32)
    place = jnp.where(
        source % 2 == row % 2,
        ((source - row) % ranks) // 2,
        near + ((source - partner) % ranks) // 2,
    ).astype(jnp.int32)

    b_local = factor_b.reshape(seqs_here, cols_here, H).transpose(0, 2, 1)
    b_local = jnp.pad(b_local, ((0, 0), (0, 0), (0, spare))).reshape(seqs_here, H * cols)
    b_near = [b_local] + [from_ahead(b_local, k) for k in range(1, near)]
    b_pieces = b_near + [to_partner(piece) for piece in b_near]
    if spare:
        pair = jnp.pad(pair, ((0, 0), (0, spare), (0, 0)))
        cotangent = jnp.pad(cotangent, ((0, 0), (0, spare), (0, 0)))
    weights = kernel_weights(
        proj_weight, proj_bias, norm_gain, norm_bias, trans_in, trans_out, cols
    )
    (new_pair, pair_grad, gb_near, gb_far), ga_pieces = pair_tile(
        place, a_pieces, b_pieces, pair, cotangent, weights, 8, 128
    )
    new_pair = new_pair[:, :cols_here]
    pair_grad = pair_grad[:, :cols_here]

    gb_pair = gb_near + to_partner(gb_far).astype(F32)
    gb_blocks = gb_pair.reshape(near, seqs_here, H * cols)
    gb_own = gb_blocks[0]
    for k in range(1, near):
        arrived = lax.ppermute(
            gb_blocks[k].astype(BF16),
            "row",
            [(r, (r + 2 * k) % ranks) for r in range(ranks)],
        )
        gb_own = gb_own + arrived.astype(F32)
    gb_own = gb_own.reshape(seqs_here, H, cols)[:, :, :cols_here].transpose(0, 2, 1)
    grad_b = gb_own.reshape(seqs_here, cols_here * H) / seq_count

    returned = [
        lax.ppermute(piece, ("row", "col"), flipped(block_pairs(k))).astype(F32)
        for k, piece in enumerate(ga_pieces)
    ]
    sums = [sum(returned[g * lines : (g + 1) * lines]) for g in range(split)]
    first = row // lines
    parts = []
    for h in range(split):
        part = sums[0]
        for g in range(1, split):
            part = jnp.where(first ^ h == g, sums[g], part)
        parts.append(part)
    grad_a = jnp.concatenate(parts, axis=1) / seq_count
    return (new_pair, pair_grad, grad_a, grad_b)


def solution(mesh):
    placed = (
        P("row", "col"),
        P("row", "col"),
        P("row", "col", None),
        P(),
        P(),
        P(),
        P(),
        P(),
        P(),
        P("row", "col", None),
    )
    return jax.shard_map(
        body,
        mesh=mesh,
        in_specs=placed,
        out_specs=(P("row", "col", None), P("row", "col", None), P("row", "col"), P("row", "col")),
        check_vma=False,
    )
```

```python
import functools

import jax
import jax.numpy as jnp
from jax import lax
from jax.experimental import pallas as pl
from jax.experimental.pallas import tpu as pltpu
from jax.sharding import PartitionSpec as P

H = 32
PARTS = (8,)
F32 = jnp.float32
BF16 = jnp.bfloat16


def mm(left, right):
    return lax.dot_general(
        left, right, (((1,), (0,)), ((), ())), preferred_element_type=F32
    )


def mm_nt(left, right):
    return lax.dot_general(
        left, right, (((1,), (1,)), ((), ())), preferred_element_type=F32
    )


ROWS = 4
BLOCK = 8
ORDER = "p0 p1 O n0 t0 n1 t1 p2 G f0 n2 p3 t2 u0 f1 n3 O t3 u1 G f2 O u2 f3 G u3"


def pair_kernel(place_ref, send_ref, *refs, ranks, lines, first, last):
    refs = list(refs)

    def take(count):
        taken = refs[:count]
        del refs[:count]
        return taken

    a_pieces = take(ranks)
    b_pieces = take(ranks)
    pair_ref, cot_ref, proj_t_ref, proj_ref, wide_ref, out_t_ref, in_ref, vec_ref = take(8)
    gb_in = None if first else take(3)[0]
    new_ref, grad_ref = take(2)
    gb_outs = take(2 if last else 1)
    ga_pieces = take(lines)
    a_s, b_ref, ga_s, gb_ref, turned_s, outer_even, outer_odd, pulled_even, pulled_odd = take(9)
    hidden_s = take(ROWS)
    both_s = take(ROWS)
    rhs_s = take(ROWS)
    step = pl.program_id(0)
    steps = pl.num_programs(0)
    seqs = b_ref.shape[0]
    share = seqs // ranks
    split = ranks // lines
    cols, width = pair_ref.shape[1:]
    units = out_t_ref.shape[1]
    chunk = units // 4
    span = BLOCK * H
    trips = BLOCK // ROWS
    per_trip = H // trips
    inv_seqs = 1.0 / seqs

    def at(index, size):
        return pl.ds(pl.multiple_of(index * size, size), size)

    def outer_pair(dest, h):
        outer = mm(turned_s[...], b_ref[:, pl.ds(pl.multiple_of(h * cols, cols), 2 * cols)])
        for k in range(2):
            half = outer[:, k * cols : (k + 1) * cols].astype(BF16)
            dest[:, at(h + k, H), :] = half.reshape(BLOCK, H, cols)

    def grad_pair(pulled, block, h):
        left = a_s[:, at(block, span)]
        total = None
        for k in range(2):
            tile = pulled[:, at(h + k, H), :].reshape(span, cols)
            lanes = at(h + k, cols)
            part = mm_nt(tile, b_ref[:, lanes])
            total = part if total is None else total + part
            gb_ref[:, lanes] += mm(left, tile)
        return total

    def put_ga(block, total):
        ga_s[...] = total.T.astype(BF16)
        for d in range(lines):
            for m in range(split):
                ga_pieces[d][m * share : (m + 1) * share, at(block, span)] = ga_s[
                    at(send_ref[d * split + m], share), :
                ]

    def half_step(outer, pulled, next_outer, next_block, last_pulled, last_block, offset):
        turned_s[...] = a_s[:, at(next_block, span)].T

        def trip(k, total):
            held = [{} for _ in range(ROWS)]
            outers = [k * per_trip + h for h in range(0, per_trip, 2)]
            grads = list(outers)
            parts = []

            def project(r):
                held[r]["projected"] = mm(proj_t_ref[...], outer[k * ROWS + r])

            def normalise(r):
                row = offset + k * ROWS + r
                updated = pair_ref[row].T.astype(F32)
                updated = updated + (held[r]["projected"] * inv_seqs + vec_ref[0])
                mean = jnp.mean(updated, axis=0, keepdims=True)
                centered = updated - mean
                var = jnp.mean(centered * centered, axis=0, keepdims=True)
                inv_std = lax.rsqrt(var + 1e-05)
                normed = centered * inv_std
                rhs_s[r][:width, :] = (normed * vec_ref[1] + vec_ref[2]).astype(BF16)
                rhs_s[r][width:, :] = cot_ref[row].T
                held[r].update(updated=updated, normed=normed, inv_std=inv_std)

            def transition(r):
                rhs = rhs_s[r][...]
                for u in range(0, units, chunk):
                    gate = mm(wide_ref[u : u + chunk, :], rhs)
                    up = mm(wide_ref[units + u : units + u + chunk, :], rhs)
                    d_hid = mm(wide_ref[2 * units + u : 2 * units + u + chunk, :], rhs)
                    sig = 0.5 * jnp.tanh(0.5 * gate) + 0.5
                    act = gate * sig
                    hidden_s[r][u : u + chunk, :] = (act * up).astype(BF16)
                    both_s[r][units + u : units + u + chunk, :] = (d_hid * act).astype(BF16)
                    d_gate = d_hid * up * (sig + act * (1.0 - sig))
                    both_s[r][u : u + chunk, :] = d_gate.astype(BF16)

            def finish(r):
                row = offset + k * ROWS + r
                normed = held[r]["normed"]
                new_t = held[r]["updated"] + mm(out_t_ref[...], hidden_s[r][...])
                new_ref[row] = new_t.astype(BF16).T
                d_norm = mm(in_ref[...], both_s[r][...]) * vec_ref[1]
                d_mean = jnp.mean(d_norm, axis=0, keepdims=True)
                d_proj = jnp.mean(d_norm * normed, axis=0, keepdims=True)
                d_norm = held[r]["inv_std"] * (d_norm - d_mean - normed * d_proj)
                grad_t = (rhs_s[r][width:, :].astype(F32) + d_norm).astype(BF16)
                held[r]["grad"] = grad_t
                grad_ref[row] = grad_t.T

            def pull(r):
                pulled[k * ROWS + r] = mm(proj_ref[...], held[r]["grad"]).astype(BF16)

            stages = {"p": project, "n": normalise, "t": transition, "f": finish, "u": pull}
            order = ORDER.split()
            for code, todo in (("O", outers), ("G", grads)):
                slots = [i for i, word in enumerate(order) if word == code]
                for j, i in enumerate(slots):
                    lo, hi = len(todo) * j // len(slots), len(todo) * (j + 1) // len(slots)
                    order[i] = (code, todo[lo:hi])
            for word in order:
                if word[0] == "O":
                    for h in word[1]:
                        outer_pair(next_outer, h)
                elif word[0] == "G":
                    for h in word[1]:
                        parts.append(grad_pair(last_pulled, last_block, h))
                else:
                    stages[word[0]](int(word[1]))
            for part in parts:
                total = total + part
            return total

        return lax.fori_loop(0, trips, trip, jnp.zeros((span, seqs), F32))

    @pl.when(step == 0)
    def _():
        gb_ref[...] = jnp.zeros_like(gb_ref) if first else gb_in[...]
        pulled_odd[...] = jnp.zeros_like(pulled_odd)
        for k in range(ranks):
            b_ref[k * share : (k + 1) * share, :] = b_pieces[k][...]
            a_s[at(place_ref[k], share), :] = a_pieces[k][...]
        turned_s[...] = a_s[:, :span].T
        for h in range(0, H, 2):
            outer_pair(outer_even, h)

    even = 2 * step
    before = jnp.maximum(even - 1, 0)
    put_ga(
        before,
        half_step(outer_even, pulled_even, outer_odd, even + 1, pulled_odd, before, 0),
    )
    after = jnp.minimum(even + 2, 2 * steps - 1)
    put_ga(even, half_step(outer_odd, pulled_odd, outer_even, after, pulled_even, even, BLOCK))

    @pl.when(step == steps - 1)
    def _():
        total = jnp.zeros((span, seqs), F32)
        for h in range(0, H, 2):
            total = total + grad_pair(pulled_odd, even + 1, h)
        put_ga(even + 1, total)
        if last:
            gb_outs[0][...] = gb_ref[: seqs // 2, :]
            gb_outs[1][...] = gb_ref[seqs // 2 :, :].astype(BF16)
        else:
            gb_outs[0][...] = gb_ref[...]


def pair_tile(place, send, a_pieces, b_pieces, pair, cot, weights, lines, start, carry, last):
    ranks = len(a_pieces)
    share, width_a = a_pieces[0].shape
    seqs = ranks * share
    _, cols, width = pair.shape
    units = weights[3].shape[1]
    step_rows = 2 * BLOCK
    base = start // step_rows

    def whole(shape):
        return pl.BlockSpec(shape, lambda b, place, send: (0,) * len(shape))

    def vmem(*shape):
        return pltpu.VMEM(shape, BF16)

    pair_spec = pl.BlockSpec((step_rows, cols, width), lambda b, place, send: (base + b, 0, 0))
    half = (seqs // 2, H * cols)
    full = (seqs, H * cols)
    piece = (seqs // lines, width_a)
    gb_shapes = [(half, F32), (half, BF16)] if last else [(full, F32)]
    carried = [] if carry is None else [whole(full)] + [pl.BlockSpec(memory_space=pl.ANY)] * 2
    inputs = [place, send, *a_pieces, *b_pieces, pair, cot, *weights]
    if carry is not None:
        aliases = {len(inputs) + 1: 0, len(inputs) + 2: 1}
        inputs += list(carry)
    else:
        aliases = {}
    outs = pl.pallas_call(
        functools.partial(
            pair_kernel, ranks=ranks, lines=lines, first=carry is None, last=last
        ),
        grid_spec=pltpu.PrefetchScalarGridSpec(
            num_scalar_prefetch=2,
            grid=(width_a // (H * step_rows),),
            in_specs=[whole(p.shape) for p in a_pieces]
            + [whole(p.shape) for p in b_pieces]
            + [pair_spec, pair_spec]
            + [whole(w.shape) for w in weights]
            + carried,
            out_specs=[pair_spec, pair_spec]
            + [whole(shape) for shape, _ in gb_shapes]
            + [whole(piece)] * lines,
            scratch_shapes=[
                vmem(seqs, width_a),
                vmem(*full),
                vmem(seqs, BLOCK * H),
                pltpu.VMEM(full, F32),
                vmem(BLOCK * H, seqs),
                *[vmem(BLOCK, H * H, cols)] * 4,
                *[vmem(units, cols)] * ROWS,
                *[vmem(2 * units, cols)] * ROWS,
                *[vmem(2 * width, cols)] * ROWS,
            ],
        ),
        out_shape=[jax.ShapeDtypeStruct(pair.shape, BF16)] * 2
        + [jax.ShapeDtypeStruct(shape, dtype) for shape, dtype in gb_shapes]
        + [jax.ShapeDtypeStruct(piece, BF16)] * lines,
        input_output_aliases=aliases,
        compiler_params=pltpu.CompilerParams(
            dimension_semantics=("arbitrary",), vmem_limit_bytes=60 * 2**20
        ),
    )(*inputs)
    cut = 2 + len(gb_shapes)
    return outs[:2], outs[2:cut], outs[cut:]


def kernel_weights(proj_weight, proj_bias, norm_gain, norm_bias, trans_in, trans_out, cols):
    width = proj_weight.shape[1]
    units = trans_out.shape[0]
    proj = proj_weight.reshape(H, H, width).transpose(1, 0, 2).reshape(H * H, width)
    wide = jnp.concatenate(
        [
            jnp.concatenate([trans_in.T, jnp.zeros((2 * units, width), BF16)], axis=1),
            jnp.concatenate([jnp.zeros((units, width), BF16), trans_out], axis=1),
        ],
        axis=0,
    )
    vec = jnp.stack([proj_bias, norm_gain, norm_bias])[:, :, None]
    vec = jnp.broadcast_to(vec, (3, width, cols))
    return proj.T, proj, wide, trans_out.T, trans_in, vec


def body(
    factor_a,
    factor_b,
    pair,
    proj_weight,
    proj_bias,
    norm_gain,
    norm_bias,
    trans_in,
    trans_out,
    cotangent,
):
    ranks = lax.axis_size("row")
    lines = lax.axis_size("col")
    split = ranks // lines
    row = lax.axis_index("row")
    col = lax.axis_index("col")
    partner = row ^ 1
    rows_here, cols_here, width = pair.shape
    seqs_here = factor_a.shape[0]
    seq_count = seqs_here * ranks
    cols = -(-cols_here // 128) * 128
    spare = cols - cols_here
    near = ranks // 2

    def to_partner(array):
        return lax.ppermute(array, "row", [(r, r ^ 1) for r in range(ranks)])

    def from_ahead(array, k):
        return lax.ppermute(array, "row", [((r + 2 * k) % ranks, r) for r in range(ranks)])

    def block_pairs(k):
        return [
            ((((r % split) * lines + c) ^ k) * lines + r // split, r * lines + c)
            for r in range(ranks)
            for c in range(lines)
        ]

    source = ((row % split) * lines + col) ^ jnp.arange(ranks, dtype=jnp.int32)
    group = (col + jnp.arange(lines, dtype=jnp.int32)) % lines
    target = group[:, None] * split + ((row % split) ^ jnp.arange(split, dtype=jnp.int32))

    def position(rank):
        mine = rank % 2 == row % 2
        ahead = (rank - jnp.where(mine, row, partner)) % ranks
        return (ahead // 2 + jnp.where(mine, 0, near)).astype(jnp.int32)

    place = position(source)
    send = position(target.reshape(ranks))

    def left_blocks(start, count):
        pieces = []
        for k in range(ranks):
            which = (row ^ k) // lines
            piece = lax.dynamic_slice_in_dim(
                factor_a, (which * rows_here + start) * H, count * H, 1
            )
            pieces.append(lax.ppermute(piece, ("row", "col"), block_pairs(k)))
        return pieces

    b_local = factor_b.reshape(seqs_here, cols_here, H).transpose(0, 2, 1)
    b_local = jnp.pad(b_local, ((0, 0), (0, 0), (0, spare))).reshape(seqs_here, H * cols)
    b_near = [b_local] + [from_ahead(b_local, k) for k in range(1, near)]
    b_pieces = b_near + [to_partner(piece) for piece in b_near]
    if spare:
        pair = jnp.pad(pair, ((0, 0), (0, spare), (0, 0)))
        cotangent = jnp.pad(cotangent, ((0, 0), (0, spare), (0, 0)))
    weights = kernel_weights(
        proj_weight, proj_bias, norm_gain, norm_bias, trans_in, trans_out, cols
    )
    def line_sum(pieces):
        total = pieces[0].astype(F32)
        for d in range(1, lines):
            ring = [(c, (c + d) % lines) for c in range(lines)]
            total = total + lax.ppermute(pieces[d], "col", ring).astype(F32)
        return total.astype(BF16)

    def to_owner(total):
        arrived = []
        for m in range(split):
            pairs = [
                (r * lines + c, (split * c + ((r % split) ^ m)) * lines + r // split)
                for r in range(ranks)
                for c in range(lines)
            ]
            block = total[m * seqs_here : (m + 1) * seqs_here]
            arrived.append(lax.ppermute(block, ("row", "col"), pairs).astype(F32))
        parts = []
        for h in range(split):
            part = arrived[0]
            for m in range(1, split):
                part = jnp.where((row % split) ^ h == m, arrived[m], part)
            parts.append(part)
        return parts

    bounds = [0]
    for part in PARTS:
        bounds.append(bounds[-1] + rows_here * part // 8)
    lefts = [left_blocks(lo, hi - lo) for lo, hi in zip(bounds, bounds[1:])]
    carry = None
    lined = []
    for i, lo in enumerate(bounds[:-1]):
        last = i == len(PARTS) - 1
        (new_pair, pair_grad), gb_outs, ga_pieces = pair_tile(
            place, send, lefts[i], b_pieces, pair, cotangent, weights, lines, lo, carry, last
        )
        carry = (*gb_outs, new_pair, pair_grad)
        lined.append(line_sum(ga_pieces))
    gb_near, gb_far = gb_outs
    new_pair = new_pair[:, :cols_here]
    pair_grad = pair_grad[:, :cols_here]

    gb_pair = gb_near + to_partner(gb_far).astype(F32)
    gb_blocks = gb_pair.reshape(near, seqs_here, H * cols)
    arrived = [
        lax.ppermute(
            gb_blocks[k].astype(BF16), "row", [(r, (r + 2 * k) % ranks) for r in range(ranks)]
        )
        for k in range(1, near)
    ]
    lined[-1], arrived = lax.optimization_barrier((lined[-1], arrived))
    gb_own = gb_blocks[0]
    for block in arrived:
        gb_own = gb_own + block.astype(F32)
    gb_own = gb_own.reshape(seqs_here, H, cols)[:, :, :cols_here].transpose(0, 2, 1)
    grad_b = gb_own.reshape(seqs_here, cols_here * H) / seq_count
    owned = [to_owner(total) for total in lined]
    grad_a = jnp.concatenate([part[h] for h in range(split) for part in owned], axis=1)
    grad_a = grad_a / seq_count
    return (new_pair, pair_grad, grad_a, grad_b)


def solution(mesh):
    placed = (
        P("row", "col"),
        P("row", "col"),
        P("row", "col", None),
        P(),
        P(),
        P(),
        P(),
        P(),
        P(),
        P("row", "col", None),
    )
    return jax.shard_map(
        body,
        mesh=mesh,
        in_specs=placed,
        out_specs=(P("row", "col", None), P("row", "col", None), P("row", "col"), P("row", "col")),
        check_vma=False,
    )
```

```python
import functools

import jax
import jax.numpy as jnp
from jax import lax
from jax.experimental import pallas as pl
from jax.experimental.pallas import tpu as pltpu
from jax.sharding import PartitionSpec as P

H = 32
PARTS = (8,)
F32 = jnp.float32
BF16 = jnp.bfloat16


def mm(left, right):
    return lax.dot_general(
        left, right, (((1,), (0,)), ((), ())), preferred_element_type=F32
    )


def mm_nt(left, right):
    return lax.dot_general(
        left, right, (((1,), (1,)), ((), ())), preferred_element_type=F32
    )


ROWS = 8
BLOCK = 8
ORDER = (
    "p0 p1 O n0 t0 n1 t1 p2 G f0 n2 t2 u0 p3 f1 n3 O t3 u1 p4 G f2 n4 t4 u2 p5 f3 n5 O t5 u3"
    " p6 G f4 n6 t6 u4 p7 f5 n7 O t7 u5 G f6 O u6 f7 G u7"
)


def pair_kernel(place_ref, send_ref, *refs, ranks, lines, first, last):
    refs = list(refs)

    def take(count):
        taken = refs[:count]
        del refs[:count]
        return taken

    a_pieces = take(ranks)
    b_pieces = take(ranks)
    pair_ref, cot_ref, proj_t_ref, proj_ref, wide_ref, out_t_ref, in_ref, vec_ref = take(8)
    gb_in = None if first else take(3)[0]
    new_ref, grad_ref = take(2)
    gb_outs = take(2 if last else 1)
    ga_pieces = take(lines)
    a_s, b_ref, ga_s, gb_ref, turned_s, outer_even, outer_odd, pulled_even, pulled_odd = take(9)
    hidden_s = take(ROWS)
    both_s = take(ROWS)
    rhs_s = take(ROWS)
    step = pl.program_id(0)
    steps = pl.num_programs(0)
    seqs = b_ref.shape[0]
    share = seqs // ranks
    split = ranks // lines
    cols, width = pair_ref.shape[1:]
    units = out_t_ref.shape[1]
    chunk = units // 4
    span = BLOCK * H
    trips = BLOCK // ROWS
    per_trip = H // trips
    inv_seqs = 1.0 / seqs

    def at(index, size):
        return pl.ds(pl.multiple_of(index * size, size), size)

    def outer_pair(dest, h):
        outer = mm(turned_s[...], b_ref[:, pl.ds(pl.multiple_of(h * cols, cols), 2 * cols)])
        for k in range(2):
            half = outer[:, k * cols : (k + 1) * cols].astype(BF16)
            dest[:, at(h + k, H), :] = half.reshape(BLOCK, H, cols)

    def grad_pair(pulled, block, h):
        left = a_s[:, at(block, span)]
        total = None
        for k in range(2):
            tile = pulled[:, at(h + k, H), :].reshape(span, cols)
            lanes = at(h + k, cols)
            part = mm_nt(tile, b_ref[:, lanes])
            total = part if total is None else total + part
            gb_ref[:, lanes] += mm(left, tile)
        return total

    def put_ga(block, total):
        ga_s[...] = total.T.astype(BF16)
        for d in range(lines):
            for m in range(split):
                ga_pieces[d][m * share : (m + 1) * share, at(block, span)] = ga_s[
                    at(send_ref[d * split + m], share), :
                ]

    def half_step(outer, pulled, next_outer, next_block, last_pulled, last_block, offset):
        turned_s[...] = a_s[:, at(next_block, span)].T

        def trip(k, total):
            held = [{} for _ in range(ROWS)]
            outers = [k * per_trip + h for h in range(0, per_trip, 2)]
            grads = list(outers)
            parts = []

            def project(r):
                held[r]["projected"] = mm(proj_t_ref[...], outer[k * ROWS + r])

            def normalise(r):
                row = offset + k * ROWS + r
                updated = pair_ref[row].T.astype(F32)
                updated = updated + (held[r]["projected"] * inv_seqs + vec_ref[0])
                mean = jnp.mean(updated, axis=0, keepdims=True)
                centered = updated - mean
                var = jnp.mean(centered * centered, axis=0, keepdims=True)
                inv_std = lax.rsqrt(var + 1e-05)
                normed = centered * inv_std
                rhs_s[r][:width, :] = (normed * vec_ref[1] + vec_ref[2]).astype(BF16)
                rhs_s[r][width:, :] = cot_ref[row].T
                held[r].update(updated=updated, normed=normed, inv_std=inv_std)

            def transition(r):
                rhs = rhs_s[r][...]
                for u in range(0, units, chunk):
                    gate = mm(wide_ref[u : u + chunk, :], rhs)
                    up = mm(wide_ref[units + u : units + u + chunk, :], rhs)
                    d_hid = mm(wide_ref[2 * units + u : 2 * units + u + chunk, :], rhs)
                    sig = 0.5 * jnp.tanh(0.5 * gate) + 0.5
                    act = gate * sig
                    hidden_s[r][u : u + chunk, :] = (act * up).astype(BF16)
                    both_s[r][units + u : units + u + chunk, :] = (d_hid * act).astype(BF16)
                    d_gate = d_hid * up * (sig + act * (1.0 - sig))
                    both_s[r][u : u + chunk, :] = d_gate.astype(BF16)

            def finish(r):
                row = offset + k * ROWS + r
                normed = held[r]["normed"]
                new_t = held[r]["updated"] + mm(out_t_ref[...], hidden_s[r][...])
                new_ref[row] = new_t.astype(BF16).T
                d_norm = mm(in_ref[...], both_s[r][...]) * vec_ref[1]
                d_mean = jnp.mean(d_norm, axis=0, keepdims=True)
                d_proj = jnp.mean(d_norm * normed, axis=0, keepdims=True)
                d_norm = held[r]["inv_std"] * (d_norm - d_mean - normed * d_proj)
                grad_t = (rhs_s[r][width:, :].astype(F32) + d_norm).astype(BF16)
                held[r]["grad"] = grad_t
                grad_ref[row] = grad_t.T

            def pull(r):
                pulled[k * ROWS + r] = mm(proj_ref[...], held[r]["grad"]).astype(BF16)

            stages = {"p": project, "n": normalise, "t": transition, "f": finish, "u": pull}
            order = ORDER.split()
            for code, todo in (("O", outers), ("G", grads)):
                slots = [i for i, word in enumerate(order) if word == code]
                for j, i in enumerate(slots):
                    lo, hi = len(todo) * j // len(slots), len(todo) * (j + 1) // len(slots)
                    order[i] = (code, todo[lo:hi])
            for word in order:
                if word[0] == "O":
                    for h in word[1]:
                        outer_pair(next_outer, h)
                elif word[0] == "G":
                    for h in word[1]:
                        parts.append(grad_pair(last_pulled, last_block, h))
                else:
                    stages[word[0]](int(word[1]))
            for part in parts:
                total = total + part
            return total

        return lax.fori_loop(0, trips, trip, jnp.zeros((span, seqs), F32))

    @pl.when(step == 0)
    def _():
        gb_ref[...] = jnp.zeros_like(gb_ref) if first else gb_in[...]
        pulled_odd[...] = jnp.zeros_like(pulled_odd)
        for k in range(ranks):
            b_ref[k * share : (k + 1) * share, :] = b_pieces[k][...]
            a_s[at(place_ref[k], share), :] = a_pieces[k][...]
        turned_s[...] = a_s[:, :span].T
        for h in range(0, H, 2):
            outer_pair(outer_even, h)

    even = 2 * step
    before = jnp.maximum(even - 1, 0)
    put_ga(
        before,
        half_step(outer_even, pulled_even, outer_odd, even + 1, pulled_odd, before, 0),
    )
    after = jnp.minimum(even + 2, 2 * steps - 1)
    put_ga(even, half_step(outer_odd, pulled_odd, outer_even, after, pulled_even, even, BLOCK))

    @pl.when(step == steps - 1)
    def _():
        total = jnp.zeros((span, seqs), F32)
        for h in range(0, H, 2):
            total = total + grad_pair(pulled_odd, even + 1, h)
        put_ga(even + 1, total)
        if last:
            gb_outs[0][...] = gb_ref[: seqs // 2, :]
            gb_outs[1][...] = gb_ref[seqs // 2 :, :].astype(BF16)
        else:
            gb_outs[0][...] = gb_ref[...]


def pair_tile(place, send, a_pieces, b_pieces, pair, cot, weights, lines, start, carry, last):
    ranks = len(a_pieces)
    share, width_a = a_pieces[0].shape
    seqs = ranks * share
    _, cols, width = pair.shape
    units = weights[3].shape[1]
    step_rows = 2 * BLOCK
    base = start // step_rows

    def whole(shape):
        return pl.BlockSpec(shape, lambda b, place, send: (0,) * len(shape))

    def vmem(*shape):
        return pltpu.VMEM(shape, BF16)

    pair_spec = pl.BlockSpec((step_rows, cols, width), lambda b, place, send: (base + b, 0, 0))
    half = (seqs // 2, H * cols)
    full = (seqs, H * cols)
    piece = (seqs // lines, width_a)
    gb_shapes = [(half, F32), (half, BF16)] if last else [(full, F32)]
    carried = [] if carry is None else [whole(full)] + [pl.BlockSpec(memory_space=pl.ANY)] * 2
    inputs = [place, send, *a_pieces, *b_pieces, pair, cot, *weights]
    if carry is not None:
        aliases = {len(inputs) + 1: 0, len(inputs) + 2: 1}
        inputs += list(carry)
    else:
        aliases = {}
    outs = pl.pallas_call(
        functools.partial(
            pair_kernel, ranks=ranks, lines=lines, first=carry is None, last=last
        ),
        grid_spec=pltpu.PrefetchScalarGridSpec(
            num_scalar_prefetch=2,
            grid=(width_a // (H * step_rows),),
            in_specs=[whole(p.shape) for p in a_pieces]
            + [whole(p.shape) for p in b_pieces]
            + [pair_spec, pair_spec]
            + [whole(w.shape) for w in weights]
            + carried,
            out_specs=[pair_spec, pair_spec]
            + [whole(shape) for shape, _ in gb_shapes]
            + [whole(piece)] * lines,
            scratch_shapes=[
                vmem(seqs, width_a),
                vmem(*full),
                vmem(seqs, BLOCK * H),
                pltpu.VMEM(full, F32),
                vmem(BLOCK * H, seqs),
                *[vmem(BLOCK, H * H, cols)] * 4,
                *[vmem(units, cols)] * ROWS,
                *[vmem(2 * units, cols)] * ROWS,
                *[vmem(2 * width, cols)] * ROWS,
            ],
        ),
        out_shape=[jax.ShapeDtypeStruct(pair.shape, BF16)] * 2
        + [jax.ShapeDtypeStruct(shape, dtype) for shape, dtype in gb_shapes]
        + [jax.ShapeDtypeStruct(piece, BF16)] * lines,
        input_output_aliases=aliases,
        compiler_params=pltpu.CompilerParams(
            dimension_semantics=("arbitrary",), vmem_limit_bytes=60 * 2**20
        ),
    )(*inputs)
    cut = 2 + len(gb_shapes)
    return outs[:2], outs[2:cut], outs[cut:]


def kernel_weights(proj_weight, proj_bias, norm_gain, norm_bias, trans_in, trans_out, cols):
    width = proj_weight.shape[1]
    units = trans_out.shape[0]
    proj = proj_weight.reshape(H, H, width).transpose(1, 0, 2).reshape(H * H, width)
    wide = jnp.concatenate(
        [
            jnp.concatenate([trans_in.T, jnp.zeros((2 * units, width), BF16)], axis=1),
            jnp.concatenate([jnp.zeros((units, width), BF16), trans_out], axis=1),
        ],
        axis=0,
    )
    vec = jnp.stack([proj_bias, norm_gain, norm_bias])[:, :, None]
    vec = jnp.broadcast_to(vec, (3, width, cols))
    return proj.T, proj, wide, trans_out.T, trans_in, vec


def body(
    factor_a,
    factor_b,
    pair,
    proj_weight,
    proj_bias,
    norm_gain,
    norm_bias,
    trans_in,
    trans_out,
    cotangent,
):
    ranks = lax.axis_size("row")
    lines = lax.axis_size("col")
    split = ranks // lines
    row = lax.axis_index("row")
    col = lax.axis_index("col")
    partner = row ^ 1
    rows_here, cols_here, width = pair.shape
    seqs_here = factor_a.shape[0]
    seq_count = seqs_here * ranks
    cols = -(-cols_here // 128) * 128
    spare = cols - cols_here
    near = ranks // 2

    def to_partner(array):
        return lax.ppermute(array, "row", [(r, r ^ 1) for r in range(ranks)])

    def from_ahead(array, k):
        return lax.ppermute(array, "row", [((r + 2 * k) % ranks, r) for r in range(ranks)])

    def block_pairs(k):
        return [
            ((((r % split) * lines + c) ^ k) * lines + r // split, r * lines + c)
            for r in range(ranks)
            for c in range(lines)
        ]

    source = ((row % split) * lines + col) ^ jnp.arange(ranks, dtype=jnp.int32)
    group = (col + jnp.arange(lines, dtype=jnp.int32)) % lines
    target = group[:, None] * split + ((row % split) ^ jnp.arange(split, dtype=jnp.int32))

    def position(rank):
        mine = rank % 2 == row % 2
        ahead = (rank - jnp.where(mine, row, partner)) % ranks
        return (ahead // 2 + jnp.where(mine, 0, near)).astype(jnp.int32)

    place = position(source)
    send = position(target.reshape(ranks))

    def left_blocks(start, count):
        pieces = []
        for k in range(ranks):
            which = (row ^ k) // lines
            piece = lax.dynamic_slice_in_dim(
                factor_a, (which * rows_here + start) * H, count * H, 1
            )
            pieces.append(lax.ppermute(piece, ("row", "col"), block_pairs(k)))
        return pieces

    b_local = factor_b.reshape(seqs_here, cols_here, H).transpose(0, 2, 1)
    b_local = jnp.pad(b_local, ((0, 0), (0, 0), (0, spare))).reshape(seqs_here, H * cols)
    b_near = [b_local] + [from_ahead(b_local, k) for k in range(1, near)]
    b_pieces = b_near + [to_partner(piece) for piece in b_near]
    if spare:
        pair = jnp.pad(pair, ((0, 0), (0, spare), (0, 0)))
        cotangent = jnp.pad(cotangent, ((0, 0), (0, spare), (0, 0)))
    weights = kernel_weights(
        proj_weight, proj_bias, norm_gain, norm_bias, trans_in, trans_out, cols
    )
    def line_sum(pieces):
        total = pieces[0].astype(F32)
        for d in range(1, lines):
            ring = [(c, (c + d) % lines) for c in range(lines)]
            total = total + lax.ppermute(pieces[d], "col", ring).astype(F32)
        return total.astype(BF16)

    def to_owner(total):
        arrived = []
        for m in range(split):
            pairs = [
                (r * lines + c, (split * c + ((r % split) ^ m)) * lines + r // split)
                for r in range(ranks)
                for c in range(lines)
            ]
            block = total[m * seqs_here : (m + 1) * seqs_here]
            arrived.append(lax.ppermute(block, ("row", "col"), pairs).astype(F32))
        parts = []
        for h in range(split):
            part = arrived[0]
            for m in range(1, split):
                part = jnp.where((row % split) ^ h == m, arrived[m], part)
            parts.append(part)
        return parts

    bounds = [0]
    for part in PARTS:
        bounds.append(bounds[-1] + rows_here * part // 8)
    lefts = [left_blocks(lo, hi - lo) for lo, hi in zip(bounds, bounds[1:])]
    carry = None
    lined = []
    for i, lo in enumerate(bounds[:-1]):
        last = i == len(PARTS) - 1
        (new_pair, pair_grad), gb_outs, ga_pieces = pair_tile(
            place, send, lefts[i], b_pieces, pair, cotangent, weights, lines, lo, carry, last
        )
        carry = (*gb_outs, new_pair, pair_grad)
        lined.append(line_sum(ga_pieces))
    gb_near, gb_far = gb_outs
    new_pair = new_pair[:, :cols_here]
    pair_grad = pair_grad[:, :cols_here]

    gb_pair = gb_near + to_partner(gb_far).astype(F32)
    gb_blocks = gb_pair.reshape(near, seqs_here, H * cols)
    arrived = [
        lax.ppermute(
            gb_blocks[k].astype(BF16), "row", [(r, (r + 2 * k) % ranks) for r in range(ranks)]
        )
        for k in range(1, near)
    ]
    lined[-1], arrived = lax.optimization_barrier((lined[-1], arrived))
    gb_own = gb_blocks[0]
    for block in arrived:
        gb_own = gb_own + block.astype(F32)
    gb_own = gb_own.reshape(seqs_here, H, cols)[:, :, :cols_here].transpose(0, 2, 1)
    grad_b = gb_own.reshape(seqs_here, cols_here * H) / seq_count
    owned = [to_owner(total) for total in lined]
    grad_a = jnp.concatenate([part[h] for h in range(split) for part in owned], axis=1)
    grad_a = grad_a / seq_count
    return (new_pair, pair_grad, grad_a, grad_b)


def solution(mesh):
    placed = (
        P("row", "col"),
        P("row", "col"),
        P("row", "col", None),
        P(),
        P(),
        P(),
        P(),
        P(),
        P(),
        P("row", "col", None),
    )
    return jax.shard_map(
        body,
        mesh=mesh,
        in_specs=placed,
        out_specs=(P("row", "col", None), P("row", "col", None), P("row", "col"), P("row", "col")),
        check_vma=False,
    )
```

```python
import functools

import jax
import jax.numpy as jnp
from jax import lax
from jax.experimental import pallas as pl
from jax.experimental.pallas import tpu as pltpu
from jax.sharding import PartitionSpec as P

H = 32
PARTS = (8,)
F32 = jnp.float32
BF16 = jnp.bfloat16


def mm(left, right):
    return lax.dot_general(
        left, right, (((1,), (0,)), ((), ())), preferred_element_type=F32
    )


def mm_nt(left, right):
    return lax.dot_general(
        left, right, (((1,), (1,)), ((), ())), preferred_element_type=F32
    )


ROWS = 8
BLOCK = 8
ORDER = (
    "p0 p1 O n0 t0 n1 t1 p2 G f0 n2 t2 u0 p3 f1 n3 O t3 u1 p4 G f2 n4 t4 u2 p5 f3 n5 O t5 u3"
    " p6 G f4 n6 t6 u4 p7 f5 n7 O t7 u5 G f6 O u6 f7 G u7"
)


def pair_kernel(place_ref, send_ref, *refs, ranks, lines, first, last):
    refs = list(refs)

    def take(count):
        taken = refs[:count]
        del refs[:count]
        return taken

    a_pieces = take(ranks)
    b_pieces = take(ranks)
    pair_ref, cot_ref, proj_t_ref, proj_ref, wide_ref, out_t_ref, in_ref, vec_ref = take(8)
    gb_in = None if first else take(3)[0]
    new_ref, grad_ref = take(2)
    gb_outs = take(2 if last else 1)
    ga_pieces = take(lines)
    a_s, b_ref, ga_s, gb_ref, turned_s, outer_even, outer_odd, pulled_even, pulled_odd = take(9)
    hidden_s = take(ROWS)
    both_s = take(ROWS)
    rhs_s = take(ROWS)
    step = pl.program_id(0)
    steps = pl.num_programs(0)
    seqs = b_ref.shape[0]
    share = seqs // ranks
    split = ranks // lines
    cols, width = pair_ref.shape[1:]
    units = out_t_ref.shape[1]
    chunk = units // 4
    span = BLOCK * H
    trips = BLOCK // ROWS
    per_trip = H // trips
    inv_seqs = 1.0 / seqs

    def at(index, size):
        return pl.ds(pl.multiple_of(index * size, size), size)

    def outer_pair(dest, h):
        outer = mm(turned_s[...], b_ref[:, pl.ds(pl.multiple_of(h * cols, cols), 2 * cols)])
        for k in range(2):
            half = outer[:, k * cols : (k + 1) * cols].astype(BF16)
            dest[:, at(h + k, H), :] = half.reshape(BLOCK, H, cols)

    def grad_pair(pulled, block, h):
        left = a_s[:, at(block, span)]
        total = None
        for k in range(2):
            tile = pulled[:, at(h + k, H), :].reshape(span, cols)
            lanes = at(h + k, cols)
            part = mm_nt(tile, b_ref[:, lanes])
            total = part if total is None else total + part
            gb_ref[:, lanes] += mm(left, tile)
        return total

    def put_ga(block, total):
        ga_s[...] = total.T.astype(BF16)
        for d in range(lines):
            for m in range(split):
                ga_pieces[d][m * share : (m + 1) * share, at(block, span)] = ga_s[
                    at(send_ref[d * split + m], share), :
                ]

    def half_step(outer, pulled, next_outer, next_block, last_pulled, last_block, offset):
        turned_s[...] = a_s[:, at(next_block, span)].T

        def trip(k, total):
            held = [{} for _ in range(ROWS)]
            outers = [k * per_trip + h for h in range(0, per_trip, 2)]
            grads = list(outers)
            parts = []

            def project(r):
                held[r]["projected"] = mm(proj_t_ref[...], outer[k * ROWS + r])

            def normalise(r):
                row = offset + k * ROWS + r
                updated = pair_ref[row].T.astype(F32)
                updated = updated + (held[r]["projected"] * inv_seqs + vec_ref[0])
                mean = jnp.mean(updated, axis=0, keepdims=True)
                centered = updated - mean
                var = jnp.mean(centered * centered, axis=0, keepdims=True)
                inv_std = lax.rsqrt(var + 1e-05)
                normed = centered * inv_std
                rhs_s[r][:width, :] = (normed * vec_ref[1] + vec_ref[2]).astype(BF16)
                rhs_s[r][width:, :] = cot_ref[row].T
                held[r].update(updated=updated, normed=normed, inv_std=inv_std)

            def transition(r):
                rhs = rhs_s[r][...]
                for u in range(0, units, chunk):
                    gate = mm(wide_ref[u : u + chunk, :], rhs)
                    up = mm(wide_ref[units + u : units + u + chunk, :], rhs)
                    d_hid = mm(wide_ref[2 * units + u : 2 * units + u + chunk, :], rhs)
                    sig = 0.5 * jnp.tanh(0.5 * gate) + 0.5
                    act = gate * sig
                    hidden_s[r][u : u + chunk, :] = (act * up).astype(BF16)
                    both_s[r][units + u : units + u + chunk, :] = (d_hid * act).astype(BF16)
                    d_gate = d_hid * up * (sig + act * (1.0 - sig))
                    both_s[r][u : u + chunk, :] = d_gate.astype(BF16)

            def finish(r):
                row = offset + k * ROWS + r
                normed = held[r]["normed"]
                new_t = held[r]["updated"] + mm(out_t_ref[...], hidden_s[r][...])
                new_ref[row] = new_t.astype(BF16).T
                d_norm = mm(in_ref[...], both_s[r][...]) * vec_ref[1]
                d_mean = jnp.mean(d_norm, axis=0, keepdims=True)
                d_proj = jnp.mean(d_norm * normed, axis=0, keepdims=True)
                d_norm = held[r]["inv_std"] * (d_norm - d_mean - normed * d_proj)
                grad_t = (rhs_s[r][width:, :].astype(F32) + d_norm).astype(BF16)
                held[r]["grad"] = grad_t
                grad_ref[row] = grad_t.T

            def pull(r):
                pulled[k * ROWS + r] = mm(proj_ref[...], held[r]["grad"]).astype(BF16)

            stages = {"p": project, "n": normalise, "t": transition, "f": finish, "u": pull}
            order = ORDER.split()
            for code, todo in (("O", outers), ("G", grads)):
                slots = [i for i, word in enumerate(order) if word == code]
                for j, i in enumerate(slots):
                    lo, hi = len(todo) * j // len(slots), len(todo) * (j + 1) // len(slots)
                    order[i] = (code, todo[lo:hi])
            for word in order:
                if word[0] == "O":
                    for h in word[1]:
                        outer_pair(next_outer, h)
                elif word[0] == "G":
                    for h in word[1]:
                        parts.append(grad_pair(last_pulled, last_block, h))
                else:
                    stages[word[0]](int(word[1]))
            for part in parts:
                total = total + part
            return total

        return lax.fori_loop(0, trips, trip, jnp.zeros((span, seqs), F32))

    @pl.when(step == 0)
    def _():
        gb_ref[...] = jnp.zeros_like(gb_ref) if first else gb_in[...]
        pulled_odd[...] = jnp.zeros_like(pulled_odd)
        for k in range(ranks):
            b_ref[k * share : (k + 1) * share, :] = b_pieces[k][...]
            a_s[at(place_ref[k], share), :] = a_pieces[k][...]
        turned_s[...] = a_s[:, :span].T
        for h in range(0, H, 2):
            outer_pair(outer_even, h)

    even = 2 * step
    before = jnp.maximum(even - 1, 0)
    put_ga(
        before,
        half_step(outer_even, pulled_even, outer_odd, even + 1, pulled_odd, before, 0),
    )
    after = jnp.minimum(even + 2, 2 * steps - 1)
    put_ga(even, half_step(outer_odd, pulled_odd, outer_even, after, pulled_even, even, BLOCK))

    @pl.when(step == steps - 1)
    def _():
        total = jnp.zeros((span, seqs), F32)
        for h in range(0, H, 2):
            total = total + grad_pair(pulled_odd, even + 1, h)
        put_ga(even + 1, total)
        if last:
            gb_outs[0][...] = gb_ref[: seqs // 2, :]
            gb_outs[1][...] = gb_ref[seqs // 2 :, :].astype(BF16)
        else:
            gb_outs[0][...] = gb_ref[...]


def pair_tile(place, send, a_pieces, b_pieces, pair, cot, weights, lines, start, carry, last):
    ranks = len(a_pieces)
    share, width_a = a_pieces[0].shape
    seqs = ranks * share
    _, cols, width = pair.shape
    units = weights[3].shape[1]
    step_rows = 2 * BLOCK
    base = start // step_rows

    def whole(shape):
        return pl.BlockSpec(shape, lambda b, place, send: (0,) * len(shape))

    def vmem(*shape):
        return pltpu.VMEM(shape, BF16)

    pair_spec = pl.BlockSpec((step_rows, cols, width), lambda b, place, send: (base + b, 0, 0))
    half = (seqs // 2, H * cols)
    full = (seqs, H * cols)
    piece = (seqs // lines, width_a)
    gb_shapes = [(half, F32), (half, BF16)] if last else [(full, F32)]
    carried = [] if carry is None else [whole(full)] + [pl.BlockSpec(memory_space=pl.ANY)] * 2
    inputs = [place, send, *a_pieces, *b_pieces, pair, cot, *weights]
    if carry is not None:
        aliases = {len(inputs) + 1: 0, len(inputs) + 2: 1}
        inputs += list(carry)
    else:
        aliases = {}
    outs = pl.pallas_call(
        functools.partial(
            pair_kernel, ranks=ranks, lines=lines, first=carry is None, last=last
        ),
        grid_spec=pltpu.PrefetchScalarGridSpec(
            num_scalar_prefetch=2,
            grid=(width_a // (H * step_rows),),
            in_specs=[whole(p.shape) for p in a_pieces]
            + [whole(p.shape) for p in b_pieces]
            + [pair_spec, pair_spec]
            + [whole(w.shape) for w in weights]
            + carried,
            out_specs=[pair_spec, pair_spec]
            + [whole(shape) for shape, _ in gb_shapes]
            + [whole(piece)] * lines,
            scratch_shapes=[
                vmem(seqs, width_a),
                vmem(*full),
                vmem(seqs, BLOCK * H),
                pltpu.VMEM(full, F32),
                vmem(BLOCK * H, seqs),
                *[vmem(BLOCK, H * H, cols)] * 4,
                *[vmem(units, cols)] * ROWS,
                *[vmem(2 * units, cols)] * ROWS,
                *[vmem(2 * width, cols)] * ROWS,
            ],
        ),
        out_shape=[jax.ShapeDtypeStruct(pair.shape, BF16)] * 2
        + [jax.ShapeDtypeStruct(shape, dtype) for shape, dtype in gb_shapes]
        + [jax.ShapeDtypeStruct(piece, BF16)] * lines,
        input_output_aliases=aliases,
        compiler_params=pltpu.CompilerParams(
            dimension_semantics=("arbitrary",), vmem_limit_bytes=60 * 2**20
        ),
    )(*inputs)
    cut = 2 + len(gb_shapes)
    return outs[:2], outs[2:cut], outs[cut:]


def kernel_weights(proj_weight, proj_bias, norm_gain, norm_bias, trans_in, trans_out, cols):
    width = proj_weight.shape[1]
    units = trans_out.shape[0]
    proj = proj_weight.reshape(H, H, width).transpose(1, 0, 2).reshape(H * H, width)
    wide = jnp.concatenate(
        [
            jnp.concatenate([trans_in.T, jnp.zeros((2 * units, width), BF16)], axis=1),
            jnp.concatenate([jnp.zeros((units, width), BF16), trans_out], axis=1),
        ],
        axis=0,
    )
    vec = jnp.stack([proj_bias, norm_gain, norm_bias])[:, :, None]
    vec = jnp.broadcast_to(vec, (3, width, cols))
    return proj.T, proj, wide, trans_out.T, trans_in, vec


def body(
    factor_a,
    factor_b,
    pair,
    proj_weight,
    proj_bias,
    norm_gain,
    norm_bias,
    trans_in,
    trans_out,
    cotangent,
):
    ranks = lax.axis_size("row")
    lines = lax.axis_size("col")
    split = ranks // lines
    row = lax.axis_index("row")
    col = lax.axis_index("col")
    partner = row ^ 1
    rows_here, cols_here, width = pair.shape
    seqs_here = factor_a.shape[0]
    seq_count = seqs_here * ranks
    cols = -(-cols_here // 128) * 128
    spare = cols - cols_here
    near = ranks // 2

    def to_partner(array):
        return lax.ppermute(array, "row", [(r, r ^ 1) for r in range(ranks)])

    def from_like(array, k):
        return lax.ppermute(array, "row", [(r ^ (2 * k), r) for r in range(ranks)])

    def block_pairs(k):
        return [
            ((((r % split) * lines + c) ^ k) * lines + r // split, r * lines + c)
            for r in range(ranks)
            for c in range(lines)
        ]

    source = ((row % split) * lines + col) ^ jnp.arange(ranks, dtype=jnp.int32)
    group = col ^ jnp.arange(lines, dtype=jnp.int32)
    target = group[:, None] * split + ((row % split) ^ jnp.arange(split, dtype=jnp.int32))

    def position(rank):
        mine = rank % 2 == row % 2
        ahead = rank ^ jnp.where(mine, row, partner)
        return (ahead // 2 + jnp.where(mine, 0, near)).astype(jnp.int32)

    place = position(source)
    send = position(target.reshape(ranks))

    def left_blocks(start, count):
        pieces = []
        for k in range(ranks):
            which = (row ^ k) // lines
            piece = lax.dynamic_slice_in_dim(
                factor_a, (which * rows_here + start) * H, count * H, 1
            )
            pieces.append(lax.ppermute(piece, ("row", "col"), block_pairs(k)))
        return pieces

    b_local = factor_b.reshape(seqs_here, cols_here, H).transpose(0, 2, 1)
    b_local = jnp.pad(b_local, ((0, 0), (0, 0), (0, spare))).reshape(seqs_here, H * cols)
    b_near = [b_local] + [from_like(b_local, k) for k in range(1, near)]
    b_pieces = b_near + [to_partner(piece) for piece in b_near]
    if spare:
        pair = jnp.pad(pair, ((0, 0), (0, spare), (0, 0)))
        cotangent = jnp.pad(cotangent, ((0, 0), (0, spare), (0, 0)))
    weights = kernel_weights(
        proj_weight, proj_bias, norm_gain, norm_bias, trans_in, trans_out, cols
    )
    def line_sum(pieces):
        total = pieces[0].astype(F32)
        for d in range(1, lines):
            ring = [(c, c ^ d) for c in range(lines)]
            total = total + lax.ppermute(pieces[d], "col", ring).astype(F32)
        return total.astype(BF16)

    def to_owner(total):
        arrived = []
        for m in range(split):
            pairs = [
                (r * lines + c, (split * c + ((r % split) ^ m)) * lines + r // split)
                for r in range(ranks)
                for c in range(lines)
            ]
            block = total[m * seqs_here : (m + 1) * seqs_here]
            arrived.append(lax.ppermute(block, ("row", "col"), pairs).astype(F32))
        parts = []
        for h in range(split):
            part = arrived[0]
            for m in range(1, split):
                part = jnp.where((row % split) ^ h == m, arrived[m], part)
            parts.append(part)
        return parts

    bounds = [0]
    for part in PARTS:
        bounds.append(bounds[-1] + rows_here * part // 8)
    lefts = [left_blocks(lo, hi - lo) for lo, hi in zip(bounds, bounds[1:])]
    carry = None
    lined = []
    for i, lo in enumerate(bounds[:-1]):
        last = i == len(PARTS) - 1
        (new_pair, pair_grad), gb_outs, ga_pieces = pair_tile(
            place, send, lefts[i], b_pieces, pair, cotangent, weights, lines, lo, carry, last
        )
        carry = (*gb_outs, new_pair, pair_grad)
        lined.append(line_sum(ga_pieces))
    gb_near, gb_far = gb_outs
    new_pair = new_pair[:, :cols_here]
    pair_grad = pair_grad[:, :cols_here]

    gb_pair = gb_near + to_partner(gb_far).astype(F32)
    gb_blocks = gb_pair.reshape(near, seqs_here, H * cols)
    arrived = [
        lax.ppermute(
            gb_blocks[k].astype(BF16), "row", [(r, r ^ (2 * k)) for r in range(ranks)]
        )
        for k in range(1, near)
    ]
    lined[-1], arrived = lax.optimization_barrier((lined[-1], arrived))
    gb_own = gb_blocks[0]
    for block in arrived:
        gb_own = gb_own + block.astype(F32)
    gb_own = gb_own.reshape(seqs_here, H, cols)[:, :, :cols_here].transpose(0, 2, 1)
    grad_b = gb_own.reshape(seqs_here, cols_here * H) / seq_count
    owned = [to_owner(total) for total in lined]
    grad_a = jnp.concatenate([part[h] for h in range(split) for part in owned], axis=1)
    grad_a = grad_a / seq_count
    return (new_pair, pair_grad, grad_a, grad_b)


def solution(mesh):
    placed = (
        P("row", "col"),
        P("row", "col"),
        P("row", "col", None),
        P(),
        P(),
        P(),
        P(),
        P(),
        P(),
        P("row", "col", None),
    )
    return jax.shard_map(
        body,
        mesh=mesh,
        in_specs=placed,
        out_specs=(P("row", "col", None), P("row", "col", None), P("row", "col"), P("row", "col")),
        check_vma=False,
    )
```
